32 devices in a mesh: grp: 2 (over core), dev: 16 (over z, y, x).
Axes of the slice: x: 2, y: 2, z: 4, core: 2. Of those that a mesh axis runs over, the one named last changes fastest.
Arguments:
- accum: float32 [4096, 24, 128], P(('grp', 'dev')), may hold values from -48 to 48
- step_count: int32 [24], replicated, may hold values from 1 to 12
- stretch_slot: int32 [4096], replicated, may hold values from 0 to 4095, as said below
- span_length: int32 [32], replicated, may hold values from 1 to 256, 4096 in all
- wet_mask: int32 [8192], P(('grp', 'dev')), may hold values 0 or 1
Outputs:
- ocean_flux: float32 [8192, 24, 128], P(('grp', 'dev'))
The draws below stay inside these ranges and needn't reach their ends.
Inputs may be any that keep to these rules, and one draw needn't show every extreme that they name: `stretch_slot`: A permutation of the slots; any 32 consecutive row blocks lie on 32 different atmosphere devices (slot // 128). `span_length`: sums to 4096; some ocean device owns exactly 256 blocks. `wet_mask`: entries of slots beyond an ocean device's span are ignored.
All inputs are finite; a program needn't handle non-finite values.
Results may differ from the reference program's by a relative error of at most 0.000071.
Values sent between devices are 32-bit elements; how exact they have to be, the bound alone decides.
A program may use at most 64 MiB of HBM per device.

```python
import math
import jax
import jax.numpy as jnp
import numpy as np

FIELDS = 24
CELLS = 128
BLOCKS_DEV = 128
DEVICE_COUNT = 32
ALL_BLOCKS = 4096
CAPACITY = 256


def draw_stretch_slot(key, part):
    devices = ALL_BLOCKS // BLOCKS_DEV
    first_key = jax.random.fold_in(key, 11)
    second_key = jax.random.fold_in(key, 12)
    dealing = jax.random.permutation(first_key, devices).astype(jnp.int32)
    rotation = jax.random.randint(second_key, (devices,), 0, BLOCKS_DEV).astype(jnp.int32)
    global_ids = jnp.arange(ALL_BLOCKS, dtype=jnp.int32)
    holder = dealing[global_ids % devices]
    local_slot = (global_ids // devices + rotation[holder]) % BLOCKS_DEV
    return (holder * BLOCKS_DEV + local_slot).astype(jnp.int32)


def set_ends(drawn, own_key, least, largest):
    extent = drawn.shape
    index_at = [jax.random.randint(jax.random.fold_in(own_key, axis), (), 0, extent[axis]) for axis in range(len(extent))]
    drawn = drawn.at[tuple(index_at)].set(least)
    longest = extent.index(max(extent))
    index_at[longest] = (index_at[longest] + 1) % extent[longest]
    return drawn.at[tuple(index_at)].set(largest)


def level_of(rng, shape, cuts, low, high):
    def one(axis_at, shards_of):
        draws = jax.random.uniform(jax.random.fold_in(jax.random.fold_in(rng, 6), axis_at), (shards_of,), jnp.float32, low / len(cuts), high / len(cuts))
        return jnp.repeat(jnp.exp(draws), shape[axis_at] // shards_of).reshape((-1,) + (1,) * (len(shape) - axis_at - 1))

    factor_of = one(*cuts[0])
    for cut in cuts[1:]:
        factor_of = factor_of * one(*cut)
    return factor_of


def profile(amount, total, limit, lean):
    weights = [(1 << 20) // math.isqrt(rank ** lean) + 1 for rank in range(2, amount + 1)]
    surplus, given = total - limit - (amount - 1), [1] * (amount - 1)
    while surplus > 0:
        free = [i for i in range(amount - 1) if given[i] < limit]
        mass, remaining = sum([weights[i] for i in free]), surplus
        for i in free:
            more = min(limit - given[i], max(1, remaining * weights[i] // mass), surplus)
            given[i] = given[i] + more
            surplus = surplus - more
    return np.array([limit] + given)


def ragged(rng, number_of, total, reach, slope):
    if number_of == 2:
        one = jax.random.randint(rng, (), max(1, total - reach), min(reach, total - 1) + 1)
        return jnp.stack([one, total - one])
    tallies = jnp.asarray(profile(number_of, total, reach, slope), jnp.int32)
    twos = (number_of - 1) // 2
    source_of, receiver = tallies[1:1 + 2 * twos:2], tallies[2:2 + 2 * twos:2]
    slack = jnp.minimum(source_of - 1, reach - receiver)
    moved = jax.random.randint(jax.random.fold_in(rng, 1), (twos,), 0, 1 << 20) % (slack + 1)
    tallies = tallies.at[1:1 + 2 * twos:2].set(source_of - moved).at[2:2 + 2 * twos:2].set(receiver + moved)
    return tallies[jax.random.permutation(jax.random.fold_in(rng, 2), number_of)]


def noise(rng, shape, scale, most, pieces=(), kind=jnp.bfloat16):
    values = jax.random.normal(rng, shape, jnp.float32) * scale
    if len(pieces) > 0:
        values = level_of(rng, shape, pieces, -0.22, 0.18) * values
    return jnp.clip(values, min=-most, max=most).astype(kind)


def setup_inputs(seed: int = 0) -> dict:
    keys = jax.random.split(jax.random.key(seed), 6)
    accum = noise(keys[0], (ALL_BLOCKS, FIELDS, CELLS), 8.0, 48.0, ((0, 32),), jnp.float32)
    step_count = set_ends(jax.random.randint(keys[1], (FIELDS,), 1, 13), jax.random.fold_in(keys[1], 1), 1, 12).astype(jnp.int32)
    stretch_slot = draw_stretch_slot(jax.random.fold_in(keys[5], 71), 0)
    span_length = ragged(keys[3], DEVICE_COUNT, ALL_BLOCKS, CAPACITY, 2).astype(jnp.int32)
    wet_mask = set_ends((jax.random.randint(keys[4], (DEVICE_COUNT * CAPACITY,), 0, 4) < 3).astype(jnp.int32), jax.random.fold_in(keys[4], 1), 0, 1)
    return dict(accum=accum, step_count=step_count, stretch_slot=stretch_slot, span_length=span_length, wet_mask=wet_mask)


def reference(accum, step_count, stretch_slot, span_length, wet_mask):
    span_end = jnp.cumsum(span_length).astype(jnp.int32)
    span_start = (span_end - span_length).astype(jnp.int32)
    global_ids = jnp.arange(ALL_BLOCKS, dtype=jnp.int32)
    owner = jnp.sum((span_end[None, :] <= global_ids[:, None]).astype(jnp.int32), axis=1).astype(jnp.int32)
    position = (owner * CAPACITY + global_ids - span_start[owner]).astype(jnp.int32)
    wet = (wet_mask[position] == 1).astype(jnp.float32)
    counts = step_count.astype(jnp.float32)
    masked = (accum[stretch_slot] / counts[None, :, None]) * wet[:, None, None]
    flat = jnp.transpose(masked, (1, 0, 2)).reshape(FIELDS, ALL_BLOCKS * CELLS)
    zero_col = jnp.zeros((FIELDS, 1), jnp.float32)
    before = jnp.concatenate([zero_col, flat[:, :-1]], axis=1)
    after_cells = jnp.concatenate([flat[:, 1:], zero_col], axis=1)
    smoothed = 0.25 * before + 0.5 * flat + 0.25 * after_cells
    smoothed = jnp.transpose(smoothed.reshape(FIELDS, ALL_BLOCKS, CELLS), (1, 0, 2)) * wet[:, None, None]
    result = jnp.zeros((DEVICE_COUNT * CAPACITY, FIELDS, CELLS), jnp.float32)
    return result.at[position].set(smoothed)
```

```python
import functools
import jax
import jax.numpy as jnp
from jax import lax
from jax.experimental import pallas as pl
from jax.experimental.pallas import tpu as pltpu
from jax.sharding import PartitionSpec as P

MESH = pl.DeviceIdType.MESH


def exchange_kernel(
    sizes, stretch, spans, wet, accum, received, halo,
    starts, packed, landed, edge_out, edge_in, send_sem, recv_sem, out_sem, edge_send, edge_recv, edge_copy,
):
    groups, chips, layers, pair_most, blocks_dev, all_blocks = sizes
    devices = groups * chips
    plane = chips // layers
    grp = lax.axis_index("grp")
    dev = lax.axis_index("dev")
    me = grp * chips + dev
    layer, place = dev // plane, dev % plane

    def at(index):
        return (index // chips, index % chips)

    barrier = pltpu.get_barrier_semaphore()

    @pl.loop(1, devices)
    def _(step):
        pl.semaphore_signal(barrier, inc=1, device_id=at((me + step) % devices), device_id_type=MESH)

    def prefix(owner, total):
        starts[owner] = total
        return total + spans[owner]

    lax.fori_loop(0, devices, prefix, jnp.int32(0))

    def find(block, found):
        return jnp.where(stretch[block] // blocks_dev == me, block, found)

    phase = lax.fori_loop(0, devices, find, jnp.int32(0), unroll=8)

    def partner(turn, rest):
        there = ((layer + turn) % layers) * plane + (place + rest % plane) % plane
        return ((grp + rest // plane) % groups) * chips + there

    def pack(owner, target, base):
        start = starts[owner]
        first = start + lax.rem(phase - start + all_blocks * devices, devices)
        for rank in range(pair_most):
            block = jnp.minimum(first + rank * devices, all_blocks - 1)
            slot = lax.rem(stretch[block], blocks_dev)
            target[base + rank] = accum[slot]

    def send_copy(other):
        return pltpu.make_async_remote_copy(
            src_ref=packed.at[pl.ds(other * pair_most, pair_most)],
            dst_ref=landed.at[pl.ds(me * pair_most, pair_most)],
            send_sem=send_sem.at[other],
            recv_sem=recv_sem.at[me],
            device_id=at(other),
            device_id_type=MESH,
        )

    def out_copy(other):
        return pltpu.make_async_copy(
            landed.at[pl.ds(other * pair_most, pair_most)],
            received.at[pl.ds(other * pair_most, pair_most)],
            out_sem.at[other],
        )

    turns = [layers // 2] + [t for t in range(1, layers) if t != layers // 2]
    if layers > 1:
        turns = turns + [0]
    else:
        turns = [0]
    rests = groups * plane
    for number, turn in enumerate(turns):
        low = 1 if turn == 0 else 0

        @pl.loop(low, rests)
        def _(rest):
            other = partner(turn, rest)
            pack(other, packed, other * pair_most)

        if number == 0:
            pl.semaphore_wait(barrier, devices - 1)

        @pl.loop(low, rests)
        def _(rest):
            send_copy(partner(turn, rest)).start()

    pack(me, landed, me * pair_most)

    for turn in reversed(turns):
        low = 1 if turn == 0 else 0

        @pl.loop(low, rests)
        def _(rest):
            other = partner(turn, rest)
            pltpu.make_async_remote_copy(
                src_ref=packed.at[pl.ds(other * pair_most, pair_most)],
                dst_ref=landed.at[pl.ds(other * pair_most, pair_most)],
                send_sem=send_sem.at[other],
                recv_sem=recv_sem.at[other],
                device_id=at(other),
                device_id_type=MESH,
            ).wait_recv()
            out_copy(other).start()

    out_copy(me).start()

    start = starts[me]
    length = spans[me]
    first_from = stretch[start] // blocks_dev
    last = jnp.maximum(length - 1, 0)
    last_from = stretch[start + last] // blocks_dev
    edge_out[0] = landed[last_from * pair_most + last // devices] * (
        wet[last] == 1
    ).astype(jnp.float32)
    edge_out[1] = landed[first_from * pair_most] * (wet[0] == 1).astype(jnp.float32)
    copies = []
    for side, shift in ((0, 1), (1, devices - 1)):
        copies.append(
            pltpu.make_async_remote_copy(
                src_ref=edge_out.at[side],
                dst_ref=edge_in.at[side],
                send_sem=edge_send.at[side],
                recv_sem=edge_recv.at[side],
                device_id=at((me + shift) % devices),
                device_id_type=MESH,
            )
        )
    for copy in copies:
        copy.start()

    @pl.loop(1, devices)
    def _(step):
        send_copy((me + step) % devices).wait_send()

    @pl.loop(0, devices)
    def _(other):
        out_copy(other).wait()

    for copy in copies:
        copy.wait()
    final = pltpu.make_async_copy(edge_in, halo, edge_copy)
    final.start()
    final.wait()


def filter_kernel(sizes, chunk, stretch, spans, wet, received, halo, recips, out, origin):
    groups, chips, pair_most, blocks_dev, all_blocks = sizes
    devices = groups * chips
    me = lax.axis_index("grp") * chips + lax.axis_index("dev")
    step = pl.program_id(0)

    @pl.when(step == 0)
    def _():
        origin[0] = lax.fori_loop(
            0, devices, lambda o, s: s + jnp.where(o < me, spans[o], 0), jnp.int32(0), unroll=8
        )

    start = origin[0]
    length = spans[me]
    capacity = wet.shape[0]
    base = step * chunk
    recip = recips[...]
    fields, cells = recip.shape
    lane = lax.broadcasted_iota(jnp.int32, (fields, cells), 1)
    at_first, at_last = lane == 0, lane == cells - 1
    left = halo[0] * recip * jnp.where(me > 0, 1.0, 0.0)
    right = halo[1] * recip * jnp.where(me < devices - 1, 1.0, 0.0)

    def wet_of(slot):
        bit = wet[jnp.clip(slot, 0, capacity - 1)] == 1
        return jnp.where(bit & (slot < length), 1.0, 0.0).astype(jnp.float32)

    def block_of(slot):
        slot = jnp.clip(slot, 0, capacity - 1)
        block = jnp.minimum(start + slot, all_blocks - 1)
        row = (stretch[block] // blocks_dev) * pair_most + slot // devices
        return received[row] * (recip * wet_of(slot))

    before = jnp.where(base == 0, left, block_of(base - 1))
    here = block_of(base)

    def one(offset, carry):
        before, here = carry
        slot = base + offset
        after = jnp.where(slot + 1 == length, right, block_of(slot + 1))
        low = pltpu.roll(jnp.where(at_last, before, here), 1, 1)
        high = pltpu.roll(jnp.where(at_first, after, here), cells - 1, 1)
        out[offset] = (0.25 * low + 0.5 * here + 0.25 * high) * wet_of(slot)
        return here, after

    lax.fori_loop(0, chunk, one, (before, here), unroll=8)


def on_device(accum, step_count, stretch_slot, span_length, wet_mask):
    groups, chips = lax.axis_size("grp"), lax.axis_size("dev")
    devices = groups * chips
    blocks_dev, fields, cells = accum.shape
    capacity = wet_mask.shape[0]
    pair_most = capacity // devices
    all_blocks = stretch_slot.shape[0]
    layers = 4 if chips % 4 == 0 else 1
    smem = pl.BlockSpec(memory_space=pltpu.SMEM)
    vmem = pl.BlockSpec(memory_space=pltpu.VMEM)
    hbm = pl.BlockSpec(memory_space=pl.ANY)
    block = (fields, cells)
    f32 = jnp.float32
    sems = pltpu.SemaphoreType.DMA
    received, halo = pl.pallas_call(
        functools.partial(
            exchange_kernel, (groups, chips, layers, pair_most, blocks_dev, all_blocks)
        ),
        out_shape=(
            jax.ShapeDtypeStruct((capacity, *block), f32),
            jax.ShapeDtypeStruct((2, *block), f32),
        ),
        in_specs=[smem, smem, smem, vmem],
        out_specs=(hbm, hbm),
        scratch_shapes=[
            pltpu.SMEM((devices,), jnp.int32),
            pltpu.VMEM((capacity, *block), f32),
            pltpu.VMEM((capacity, *block), f32),
            pltpu.VMEM((2, *block), f32),
            pltpu.VMEM((2, *block), f32),
            sems((devices,)),
            sems((devices,)),
            sems((devices,)),
            sems((2,)),
            sems((2,)),
            sems,
        ],
        compiler_params=pltpu.CompilerParams(collective_id=0, has_side_effects=True),
    )(stretch_slot, span_length, wet_mask, accum)
    recips = jnp.broadcast_to((1.0 / step_count.astype(f32))[:, None], block)
    chunk = 32 if capacity % 32 == 0 else capacity
    return pl.pallas_call(
        functools.partial(
            filter_kernel, (groups, chips, pair_most, blocks_dev, all_blocks), chunk
        ),
        grid=(capacity // chunk,),
        out_shape=jax.ShapeDtypeStruct((capacity, *block), f32),
        in_specs=[smem, smem, smem, vmem, vmem, vmem],
        out_specs=pl.BlockSpec((chunk, *block), lambda step: (step, 0, 0)),
        scratch_shapes=[pltpu.SMEM((1,), jnp.int32)],
    )(stretch_slot, span_length, wet_mask, received, halo, recips)


def solution(mesh):
    return jax.shard_map(
        on_device,
        mesh=mesh,
        in_specs=(P(("grp", "dev"), None, None), P(), P(), P(), P(("grp", "dev"))),
        out_specs=P(("grp", "dev"), None, None),
        check_vma=False,
    )
```

```python
import functools
import jax
import jax.numpy as jnp
from jax import lax
from jax.experimental import pallas as pl
from jax.experimental.pallas import tpu as pltpu
from jax.sharding import PartitionSpec as P

MESH = pl.DeviceIdType.MESH
ROOMS = (10, 12)


def exchange_kernel(
    sizes, stretch, spans, wet, accum, received, halo,
    starts, packed, landed, edge_out, edge_in, send_sem, recv_sem, out_sem, edge_send, edge_recv, edge_copy,
):
    groups, chips, layers, pair_most, blocks_dev, all_blocks = sizes
    devices = groups * chips
    plane = chips // layers
    grp = lax.axis_index("grp")
    dev = lax.axis_index("dev")
    me = grp * chips + dev
    layer, place = dev // plane, dev % plane

    def at(index):
        return (index // chips, index % chips)

    barrier = pltpu.get_barrier_semaphore()

    @pl.loop(1, devices)
    def _(step):
        pl.semaphore_signal(barrier, inc=1, device_id=at((me + step) % devices), device_id_type=MESH)

    def prefix(owner, total):
        starts[owner] = total
        return total + spans[owner]

    lax.fori_loop(0, devices, prefix, jnp.int32(0))

    def find(block, found):
        return jnp.where(stretch[block] // blocks_dev == me, block, found)

    phase = lax.fori_loop(0, devices, find, jnp.int32(0), unroll=8)

    def partner(turn, rest):
        there = ((layer + turn) % layers) * plane + (place + rest % plane) % plane
        return ((grp + rest // plane) % groups) * chips + there

    def pack(owner, target, base):
        start = starts[owner]
        first = start + lax.rem(phase - start + all_blocks * devices, devices)
        for rank in range(pair_most):
            block = jnp.minimum(first + rank * devices, all_blocks - 1)
            slot = lax.rem(stretch[block], blocks_dev)
            target[base + rank] = accum[slot]

    def send_copy(other):
        return pltpu.make_async_remote_copy(
            src_ref=packed.at[pl.ds(other * pair_most, pair_most)],
            dst_ref=landed.at[pl.ds(me * pair_most, pair_most)],
            send_sem=send_sem.at[other],
            recv_sem=recv_sem.at[me],
            device_id=at(other),
            device_id_type=MESH,
        )

    def out_copy(other):
        return pltpu.make_async_copy(
            landed.at[pl.ds(other * pair_most, pair_most)],
            received.at[pl.ds(other * pair_most, pair_most)],
            out_sem.at[other],
        )

    turns = [layers // 2] + [t for t in range(1, layers) if t != layers // 2]
    if layers > 1:
        turns = turns + [0]
    else:
        turns = [0]
    rests = groups * plane
    for number, turn in enumerate(turns):
        low = 1 if turn == 0 else 0

        @pl.loop(low, rests)
        def _(rest):
            other = partner(turn, rest)
            pack(other, packed, other * pair_most)

        if number == 0:
            pl.semaphore_wait(barrier, devices - 1)

        @pl.loop(low, rests)
        def _(rest):
            send_copy(partner(turn, rest)).start()

    pack(me, landed, me * pair_most)

    for turn in reversed(turns):
        low = 1 if turn == 0 else 0

        @pl.loop(low, rests)
        def _(rest):
            other = partner(turn, rest)
            pltpu.make_async_remote_copy(
                src_ref=packed.at[pl.ds(other * pair_most, pair_most)],
                dst_ref=landed.at[pl.ds(other * pair_most, pair_most)],
                send_sem=send_sem.at[other],
                recv_sem=recv_sem.at[other],
                device_id=at(other),
                device_id_type=MESH,
            ).wait_recv()
            out_copy(other).start()

    out_copy(me).start()

    start = starts[me]
    length = spans[me]
    first_from = stretch[start] // blocks_dev
    last = jnp.maximum(length - 1, 0)
    last_from = stretch[start + last] // blocks_dev
    edge_out[0] = landed[last_from * pair_most + last // devices] * (
        wet[last] == 1
    ).astype(jnp.float32)
    edge_out[1] = landed[first_from * pair_most] * (wet[0] == 1).astype(jnp.float32)
    copies = []
    for side, shift in ((0, 1), (1, devices - 1)):
        copies.append(
            pltpu.make_async_remote_copy(
                src_ref=edge_out.at[side],
                dst_ref=edge_in.at[side],
                send_sem=edge_send.at[side],
                recv_sem=edge_recv.at[side],
                device_id=at((me + shift) % devices),
                device_id_type=MESH,
            )
        )
    for copy in copies:
        copy.start()

    @pl.loop(1, devices)
    def _(step):
        send_copy((me + step) % devices).wait_send()

    @pl.loop(0, devices)
    def _(other):
        out_copy(other).wait()

    for copy in copies:
        copy.wait()
    final = pltpu.make_async_copy(edge_in, halo, edge_copy)
    final.start()
    final.wait()


def relay_kernel(
    sizes, room, stretch, spans, wet, accum, received, halo,
    starts, packed, relay_one, relay_two, relay_three, forward, landed, edge_out, edge_in,
    far_send, far_recv, send_sem, recv_sem, out_sem, edge_send, edge_recv, edge_copy,
):
    groups, chips, layers, pair_most, blocks_dev, all_blocks = sizes
    devices = groups * chips
    plane = chips // layers
    rests = groups * plane
    relayed = (None, relay_one, relay_two, relay_three)
    grp = lax.axis_index("grp")
    dev = lax.axis_index("dev")
    me = grp * chips + dev
    layer, place = dev // plane, dev % plane
    across = (layer, layer + 1 - 2 * (layer % 2), (layer + 2) % 4, 3 - layer)

    def at(index):
        return (index // chips, index % chips)

    barrier = pltpu.get_barrier_semaphore()

    @pl.loop(1, devices)
    def _(step):
        pl.semaphore_signal(barrier, inc=1, device_id=at((me + step) % devices), device_id_type=MESH)

    def prefix(owner, total):
        starts[owner] = total
        return total + spans[owner]

    starts[devices] = lax.fori_loop(0, devices, prefix, jnp.int32(0))

    def find(block, found):
        holder = stretch[block] // blocks_dev
        base = grp * chips + place
        return tuple(
            jnp.where(holder == base + across[turn] * plane, block, found[turn]) for turn in range(4)
        )

    phases = lax.fori_loop(0, devices, find, (jnp.int32(0),) * 4, unroll=8)

    def first_of(phase, start):
        return start + lax.rem(phase - start + all_blocks * devices, devices)

    def ranges(phase, target):
        firsts, amount = [], None
        for part in range(2):
            low = part * chips + target * plane
            first = first_of(phase, starts[low])
            firsts.append(first)
            if part == 0:
                amount = (starts[low + plane] - first + devices - 1) // devices
        return firsts, amount

    def slot_of(block):
        return lax.rem(stretch[jnp.minimum(block, all_blocks - 1)], blocks_dev)

    def far_copy(turn):
        return pltpu.make_async_remote_copy(
            src_ref=packed.at[turn - 1],
            dst_ref=relayed[turn],
            send_sem=far_send.at[turn - 1],
            recv_sem=far_recv.at[turn - 1],
            device_id=at(grp * chips + across[turn] * plane + place),
            device_id_type=MESH,
        )

    for turn in (1, 2, 3):
        (first_low, first_high), amount = ranges(phases[0], across[turn])

        def fill(spot, carry, turn=turn, first_low=first_low, first_high=first_high, amount=amount):
            block = jnp.where(
                spot < amount, first_low + devices * spot, first_high + devices * (spot - amount)
            )
            packed[turn - 1, spot] = accum[slot_of(block)]
            return carry

        lax.fori_loop(0, room, fill, jnp.int32(0), unroll=4)
        if turn == 1:
            pl.semaphore_wait(barrier, devices - 1)
        far_copy(turn).start()

    def mate(rest):
        return ((grp + rest // plane) % groups) * chips + layer * plane + (place + rest % plane) % plane

    def shifted(index, turn):
        return index + (across[turn] - layer) * plane

    def near_copy(turn, rest, sender):
        return pltpu.make_async_remote_copy(
            src_ref=forward.at[pl.ds((turn * rests + rest) * pair_most, pair_most)],
            dst_ref=landed.at[pl.ds(sender * pair_most, pair_most)],
            send_sem=send_sem.at[turn * rests + rest],
            recv_sem=recv_sem.at[sender],
            device_id=at(mate(rest)),
            device_id_type=MESH,
        )

    def out_copy(other):
        return pltpu.make_async_copy(
            landed.at[pl.ds(other * pair_most, pair_most)],
            received.at[pl.ds(other * pair_most, pair_most)],
            out_sem.at[other],
        )

    def hand_on(turn):
        phase = phases[turn]
        sender = shifted(me, turn)
        if turn > 0:
            (first_low, first_high), amount = ranges(phase, layer)

        def put(owner, target, base):
            first = first_of(phase, starts[owner])
            if turn == 0:
                for rank in range(pair_most):
                    target[base + rank] = accum[slot_of(first + rank * devices)]
            else:
                in_low = owner < chips
                spot = jnp.where(in_low, first - first_low, first - first_high) // devices
                spot = spot + jnp.where(in_low, 0, amount)
                for rank in range(pair_most):
                    target[base + rank] = relayed[turn][jnp.clip(spot + rank, 0, room - 1)]

        @pl.loop(1, rests)
        def _(rest):
            put(mate(rest), forward, (turn * rests + rest) * pair_most)

        @pl.loop(1, rests)
        def _(rest):
            near_copy(turn, rest, sender).start()

        put(me, landed, sender * pair_most)

    def take(turn):
        out_copy(shifted(me, turn)).start()

        @pl.loop(1, rests)
        def _(rest):
            sender = shifted(mate(rest), turn)
            near_copy(turn, rest, sender).wait_recv()
            out_copy(sender).start()

    hand_on(0)
    for turn in (1, 2, 3):
        far_copy(turn).wait_recv()
        hand_on(turn)
        take(turn - 1)
    take(3)

    start = starts[me]
    length = spans[me]
    first_from = stretch[start] // blocks_dev
    last = jnp.maximum(length - 1, 0)
    last_from = stretch[start + last] // blocks_dev
    edge_out[0] = landed[last_from * pair_most + last // devices] * (
        wet[last] == 1
    ).astype(jnp.float32)
    edge_out[1] = landed[first_from * pair_most] * (wet[0] == 1).astype(jnp.float32)
    copies = []
    for side, shift in ((0, 1), (1, devices - 1)):
        copies.append(
            pltpu.make_async_remote_copy(
                src_ref=edge_out.at[side],
                dst_ref=edge_in.at[side],
                send_sem=edge_send.at[side],
                recv_sem=edge_recv.at[side],
                device_id=at((me + shift) % devices),
                device_id_type=MESH,
            )
        )
    for copy in copies:
        copy.start()
    for turn in range(4):
        if turn > 0:
            far_copy(turn).wait_send()

        @pl.loop(1, rests)
        def _(rest):
            near_copy(turn, rest, me).wait_send()

    @pl.loop(0, devices)
    def _(other):
        out_copy(other).wait()

    for copy in copies:
        copy.wait()
    final = pltpu.make_async_copy(edge_in, halo, edge_copy)
    final.start()
    final.wait()


def filter_kernel(sizes, chunk, stretch, spans, wet, received, halo, recips, out, origin):
    groups, chips, pair_most, blocks_dev, all_blocks = sizes
    devices = groups * chips
    me = lax.axis_index("grp") * chips + lax.axis_index("dev")
    step = pl.program_id(0)

    @pl.when(step == 0)
    def _():
        origin[0] = lax.fori_loop(
            0, devices, lambda o, s: s + jnp.where(o < me, spans[o], 0), jnp.int32(0), unroll=8
        )

    start = origin[0]
    length = spans[me]
    capacity = wet.shape[0]
    base = step * chunk
    recip = recips[...]
    fields, cells = recip.shape
    lane = lax.broadcasted_iota(jnp.int32, (fields, cells), 1)
    at_first, at_last = lane == 0, lane == cells - 1
    left = halo[0] * recip * jnp.where(me > 0, 1.0, 0.0)
    right = halo[1] * recip * jnp.where(me < devices - 1, 1.0, 0.0)

    def wet_of(slot):
        bit = wet[jnp.clip(slot, 0, capacity - 1)] == 1
        return jnp.where(bit & (slot < length), 1.0, 0.0).astype(jnp.float32)

    def block_of(slot):
        slot = jnp.clip(slot, 0, capacity - 1)
        block = jnp.minimum(start + slot, all_blocks - 1)
        row = (stretch[block] // blocks_dev) * pair_most + slot // devices
        return received[row] * (recip * wet_of(slot))

    before = jnp.where(base == 0, left, block_of(base - 1))
    here = block_of(base)

    def one(offset, carry):
        before, here = carry
        slot = base + offset
        after = jnp.where(slot + 1 == length, right, block_of(slot + 1))
        low = pltpu.roll(jnp.where(at_last, before, here), 1, 1)
        high = pltpu.roll(jnp.where(at_first, after, here), cells - 1, 1)
        out[offset] = (0.25 * low + 0.5 * here + 0.25 * high) * wet_of(slot)
        return here, after

    lax.fori_loop(0, chunk, one, (before, here), unroll=8)


def on_device(accum, step_count, stretch_slot, span_length, wet_mask):
    groups, chips = lax.axis_size("grp"), lax.axis_size("dev")
    devices = groups * chips
    blocks_dev, fields, cells = accum.shape
    capacity = wet_mask.shape[0]
    pair_most = capacity // devices
    all_blocks = stretch_slot.shape[0]
    layers = 4 if chips % 4 == 0 else 1
    smem = pl.BlockSpec(memory_space=pltpu.SMEM)
    vmem = pl.BlockSpec(memory_space=pltpu.VMEM)
    hbm = pl.BlockSpec(memory_space=pl.ANY)
    block = (fields, cells)
    f32 = jnp.float32
    sems = pltpu.SemaphoreType.DMA
    rows = pltpu.VMEM((capacity, *block), f32)
    pair = pltpu.VMEM((2, *block), f32)
    operands = (stretch_slot, span_length, wet_mask, accum)
    sizes = (groups, chips, layers, pair_most, blocks_dev, all_blocks)

    def exchange(kernel, scratch, number):
        return pl.pallas_call(
            kernel,
            out_shape=(
                jax.ShapeDtypeStruct((capacity, *block), f32),
                jax.ShapeDtypeStruct((2, *block), f32),
            ),
            in_specs=[smem, smem, smem, vmem],
            out_specs=(hbm, hbm),
            scratch_shapes=scratch,
            compiler_params=pltpu.CompilerParams(collective_id=number, has_side_effects=True),
        )

    def direct(*given):
        scratch = [pltpu.SMEM((devices,), jnp.int32), rows, rows, pair, pair]
        scratch += [sems((devices,))] * 3 + [sems((2,)), sems((2,)), sems]
        return exchange(functools.partial(exchange_kernel, sizes), scratch, 0)(*given)

    def relay(number, room):
        def run(*given):
            one = pltpu.VMEM((room, *block), f32)
            rests = devices // layers
            scratch = [pltpu.SMEM((devices + 1,), jnp.int32), pltpu.VMEM((3, room, *block), f32)]
            scratch += [one, one, one, pltpu.VMEM((4 * rests * pair_most, *block), f32), rows, pair, pair]
            scratch += [sems((3,)), sems((3,)), sems((4 * rests,)), sems((devices,)), sems((devices,))]
            scratch += [sems((2,)), sems((2,)), sems]
            return exchange(functools.partial(relay_kernel, sizes, room), scratch, number)(*given)

        return run

    if layers == 4 and groups == 2 and pair_most >= 8:
        most = (devices // layers) * pair_most
        rooms = [most * part // 16 for part in ROOMS]
        parts = jnp.sum(span_length.reshape(groups, layers, chips // layers), axis=2)
        need = jnp.max(jnp.sum((parts + devices - 1) // devices, axis=0))
        choice = sum((need > room).astype(jnp.int32) for room in rooms)
        branches = [relay(number + 1, room) for number, room in enumerate(rooms)] + [direct]
        received, halo = lax.switch(choice, branches, *operands)
    else:
        received, halo = direct(*operands)
    recips = jnp.broadcast_to((1.0 / step_count.astype(f32))[:, None], block)
    chunk = 32 if capacity % 32 == 0 else capacity
    return pl.pallas_call(
        functools.partial(
            filter_kernel, (groups, chips, pair_most, blocks_dev, all_blocks), chunk
        ),
        grid=(capacity // chunk,),
        out_shape=jax.ShapeDtypeStruct((capacity, *block), f32),
        in_specs=[smem, smem, smem, vmem, vmem, vmem],
        out_specs=pl.BlockSpec((chunk, *block), lambda step: (step, 0, 0)),
        scratch_shapes=[pltpu.SMEM((1,), jnp.int32)],
    )(stretch_slot, span_length, wet_mask, received, halo, recips)


def solution(mesh):
    return jax.shard_map(
        on_device,
        mesh=mesh,
        in_specs=(P(("grp", "dev"), None, None), P(), P(), P(), P(("grp", "dev"))),
        out_specs=P(("grp", "dev"), None, None),
        check_vma=False,
    )
```

```python
import functools
import jax
import jax.numpy as jnp
from jax import lax
from jax.experimental import pallas as pl
from jax.experimental.pallas import tpu as pltpu
from jax.sharding import PartitionSpec as P

MESH = pl.DeviceIdType.MESH
ROOMS = (36, 38, 40, 42, 44, 48)


def exchange_kernel(
    sizes, stretch, spans, wet, accum, received, halo,
    starts, packed, landed, edge_out, edge_in, send_sem, recv_sem, out_sem, edge_send, edge_recv, edge_copy,
):
    groups, chips, layers, pair_most, blocks_dev, all_blocks = sizes
    devices = groups * chips
    plane = chips // layers
    grp = lax.axis_index("grp")
    dev = lax.axis_index("dev")
    me = grp * chips + dev
    layer, place = dev // plane, dev % plane

    def at(index):
        return (index // chips, index % chips)

    barrier = pltpu.get_barrier_semaphore()

    @pl.loop(1, devices)
    def _(step):
        pl.semaphore_signal(barrier, inc=1, device_id=at((me + step) % devices), device_id_type=MESH)

    def prefix(owner, total):
        starts[owner] = total
        return total + spans[owner]

    lax.fori_loop(0, devices, prefix, jnp.int32(0))

    def find(block, found):
        return jnp.where(stretch[block] // blocks_dev == me, block, found)

    phase = lax.fori_loop(0, devices, find, jnp.int32(0), unroll=8)

    def partner(turn, rest):
        there = ((layer + turn) % layers) * plane + (place + rest % plane) % plane
        return ((grp + rest // plane) % groups) * chips + there

    def pack(owner, target, base):
        start = starts[owner]
        first = start + lax.rem(phase - start + all_blocks * devices, devices)
        for rank in range(pair_most):
            block = jnp.minimum(first + rank * devices, all_blocks - 1)
            slot = lax.rem(stretch[block], blocks_dev)
            target[base + rank] = accum[slot]

    def send_copy(other):
        return pltpu.make_async_remote_copy(
            src_ref=packed.at[pl.ds(other * pair_most, pair_most)],
            dst_ref=landed.at[pl.ds(me * pair_most, pair_most)],
            send_sem=send_sem.at[other],
            recv_sem=recv_sem.at[me],
            device_id=at(other),
            device_id_type=MESH,
        )

    def out_copy(other):
        return pltpu.make_async_copy(
            landed.at[pl.ds(other * pair_most, pair_most)],
            received.at[pl.ds(other * pair_most, pair_most)],
            out_sem.at[other],
        )

    turns = [layers // 2] + [t for t in range(1, layers) if t != layers // 2]
    if layers > 1:
        turns = turns + [0]
    else:
        turns = [0]
    rests = groups * plane
    for number, turn in enumerate(turns):
        low = 1 if turn == 0 else 0

        @pl.loop(low, rests)
        def _(rest):
            other = partner(turn, rest)
            pack(other, packed, other * pair_most)

        if number == 0:
            pl.semaphore_wait(barrier, devices - 1)

        @pl.loop(low, rests)
        def _(rest):
            send_copy(partner(turn, rest)).start()

    pack(me, landed, me * pair_most)

    for turn in reversed(turns):
        low = 1 if turn == 0 else 0

        @pl.loop(low, rests)
        def _(rest):
            other = partner(turn, rest)
            pltpu.make_async_remote_copy(
                src_ref=packed.at[pl.ds(other * pair_most, pair_most)],
                dst_ref=landed.at[pl.ds(other * pair_most, pair_most)],
                send_sem=send_sem.at[other],
                recv_sem=recv_sem.at[other],
                device_id=at(other),
                device_id_type=MESH,
            ).wait_recv()
            out_copy(other).start()

    out_copy(me).start()

    start = starts[me]
    length = spans[me]
    first_from = stretch[start] // blocks_dev
    last = jnp.maximum(length - 1, 0)
    last_from = stretch[start + last] // blocks_dev
    edge_out[0] = landed[last_from * pair_most + last // devices] * (
        wet[last] == 1
    ).astype(jnp.float32)
    edge_out[1] = landed[first_from * pair_most] * (wet[0] == 1).astype(jnp.float32)
    copies = []
    for side, shift in ((0, 1), (1, devices - 1)):
        copies.append(
            pltpu.make_async_remote_copy(
                src_ref=edge_out.at[side],
                dst_ref=edge_in.at[side],
                send_sem=edge_send.at[side],
                recv_sem=edge_recv.at[side],
                device_id=at((me + shift) % devices),
                device_id_type=MESH,
            )
        )
    for copy in copies:
        copy.start()

    @pl.loop(1, devices)
    def _(step):
        send_copy((me + step) % devices).wait_send()

    @pl.loop(0, devices)
    def _(other):
        out_copy(other).wait()

    for copy in copies:
        copy.wait()
    final = pltpu.make_async_copy(edge_in, halo, edge_copy)
    final.start()
    final.wait()


def relay_kernel(
    sizes, room, stretch, spans, wet, accum, received, halo,
    starts, packed, relay_one, relay_two, relay_three, forward, landed, edge_out, edge_in,
    far_send, far_recv, send_sem, recv_sem, out_sem, edge_send, edge_recv, edge_copy,
):
    groups, chips, layers, pair_most, blocks_dev, all_blocks = sizes
    devices = groups * chips
    plane = chips // layers
    rests = groups * plane
    relayed = (None, relay_one, relay_two, relay_three)
    grp = lax.axis_index("grp")
    dev = lax.axis_index("dev")
    me = grp * chips + dev
    layer, place = dev // plane, dev % plane
    across = (layer, layer + 1 - 2 * (layer % 2), (layer + 2) % 4, 3 - layer)

    def at(index):
        return (index // chips, index % chips)

    barrier = pltpu.get_barrier_semaphore()

    @pl.loop(1, devices)
    def _(step):
        pl.semaphore_signal(barrier, inc=1, device_id=at((me + step) % devices), device_id_type=MESH)

    def prefix(owner, total):
        starts[owner] = total
        return total + spans[owner]

    starts[devices] = lax.fori_loop(0, devices, prefix, jnp.int32(0))

    def find(block, found):
        holder = stretch[block] // blocks_dev
        base = grp * chips + place
        return tuple(
            jnp.where(holder == base + across[turn] * plane, block, found[turn]) for turn in range(4)
        )

    phases = lax.fori_loop(0, devices, find, (jnp.int32(0),) * 4, unroll=8)

    def first_of(phase, start):
        return start + lax.rem(phase - start + all_blocks * devices, devices)

    def ranges(phase, target):
        firsts, amount = [], None
        for part in range(2):
            low = part * chips + target * plane
            first = first_of(phase, starts[low])
            firsts.append(first)
            if part == 0:
                amount = (starts[low + plane] - first + devices - 1) // devices
        return firsts, amount

    def slot_of(block):
        return lax.rem(stretch[jnp.minimum(block, all_blocks - 1)], blocks_dev)

    def far_copy(turn):
        return pltpu.make_async_remote_copy(
            src_ref=packed.at[turn - 1],
            dst_ref=relayed[turn],
            send_sem=far_send.at[turn - 1],
            recv_sem=far_recv.at[turn - 1],
            device_id=at(grp * chips + across[turn] * plane + place),
            device_id_type=MESH,
        )

    for turn in (1, 2, 3):
        (first_low, first_high), amount = ranges(phases[0], across[turn])

        def fill(spot, carry, turn=turn, first_low=first_low, first_high=first_high, amount=amount):
            block = jnp.where(
                spot < amount, first_low + devices * spot, first_high + devices * (spot - amount)
            )
            packed[turn - 1, spot] = accum[slot_of(block)]
            return carry

        lax.fori_loop(0, room, fill, jnp.int32(0), unroll=2)
        if turn == 1:
            pl.semaphore_wait(barrier, devices - 1)
        far_copy(turn).start()

    def mate(rest):
        return ((grp + rest // plane) % groups) * chips + layer * plane + (place + rest % plane) % plane

    def shifted(index, turn):
        return index + (across[turn] - layer) * plane

    def near_copy(turn, rest, sender):
        return pltpu.make_async_remote_copy(
            src_ref=forward.at[pl.ds((turn * rests + rest) * pair_most, pair_most)],
            dst_ref=landed.at[pl.ds(sender * pair_most, pair_most)],
            send_sem=send_sem.at[turn * rests + rest],
            recv_sem=recv_sem.at[sender],
            device_id=at(mate(rest)),
            device_id_type=MESH,
        )

    def out_copy(other):
        return pltpu.make_async_copy(
            landed.at[pl.ds(other * pair_most, pair_most)],
            received.at[pl.ds(other * pair_most, pair_most)],
            out_sem.at[other],
        )

    def hand_on(turn):
        phase = phases[turn]
        sender = shifted(me, turn)
        if turn > 0:
            (first_low, first_high), amount = ranges(phase, layer)

        def put(owner, target, base):
            first = first_of(phase, starts[owner])
            if turn == 0:
                for rank in range(pair_most):
                    target[base + rank] = accum[slot_of(first + rank * devices)]
            else:
                in_low = owner < chips
                spot = jnp.where(in_low, first - first_low, first - first_high) // devices
                spot = spot + jnp.where(in_low, 0, amount)
                for rank in range(pair_most):
                    target[base + rank] = relayed[turn][jnp.clip(spot + rank, 0, room - 1)]

        @pl.loop(1, rests)
        def _(rest):
            put(mate(rest), forward, (turn * rests + rest) * pair_most)

        @pl.loop(1, rests)
        def _(rest):
            near_copy(turn, rest, sender).start()

        put(me, landed, sender * pair_most)

    def take(turn):
        out_copy(shifted(me, turn)).start()

        @pl.loop(1, rests)
        def _(rest):
            sender = shifted(mate(rest), turn)
            near_copy(turn, rest, sender).wait_recv()
            out_copy(sender).start()

    hand_on(0)
    for turn in (1, 2, 3):
        far_copy(turn).wait_recv()
        hand_on(turn)
        take(turn - 1)
    take(3)

    start = starts[me]
    length = spans[me]
    first_from = stretch[start] // blocks_dev
    last = jnp.maximum(length - 1, 0)
    last_from = stretch[start + last] // blocks_dev
    edge_out[0] = landed[last_from * pair_most + last // devices] * (
        wet[last] == 1
    ).astype(jnp.float32)
    edge_out[1] = landed[first_from * pair_most] * (wet[0] == 1).astype(jnp.float32)
    copies = []
    for side, shift in ((0, 1), (1, devices - 1)):
        copies.append(
            pltpu.make_async_remote_copy(
                src_ref=edge_out.at[side],
                dst_ref=edge_in.at[side],
                send_sem=edge_send.at[side],
                recv_sem=edge_recv.at[side],
                device_id=at((me + shift) % devices),
                device_id_type=MESH,
            )
        )
    for copy in copies:
        copy.start()
    for turn in range(4):
        if turn > 0:
            far_copy(turn).wait_send()

        @pl.loop(1, rests)
        def _(rest):
            near_copy(turn, rest, me).wait_send()

    @pl.loop(0, devices)
    def _(other):
        out_copy(other).wait()

    for copy in copies:
        copy.wait()
    final = pltpu.make_async_copy(edge_in, halo, edge_copy)
    final.start()
    final.wait()


def filter_kernel(sizes, chunk, stretch, spans, wet, counts, received, halo, out, rows, recips):
    groups, chips, pair_most, blocks_dev, all_blocks = sizes
    devices = groups * chips
    me = lax.axis_index("grp") * chips + lax.axis_index("dev")
    step = pl.program_id(0)
    length = spans[me]
    capacity = wet.shape[0]
    _, fields, cells = halo.shape

    @pl.when(step == 0)
    def _():
        start = lax.fori_loop(
            0, devices, lambda o, s: s + jnp.where(o < me, spans[o], 0), jnp.int32(0), unroll=8
        )

        def fill(spot, carry):
            rows[spot] = (stretch[jnp.minimum(start + spot, all_blocks - 1)] // blocks_dev) * pair_most
            return carry

        lax.fori_loop(0, devices, fill, jnp.int32(0), unroll=8)
        field = lax.broadcasted_iota(jnp.int32, (fields, cells), 0)
        held = jnp.ones((fields, cells), jnp.int32)
        for index in range(fields):
            held = jnp.where(field == index, counts[index], held)
        recips[...] = 0.25 / held.astype(jnp.float32)

    base = step * chunk
    scale = recips[...]
    lane = lax.broadcasted_iota(jnp.int32, (fields, cells), 1)
    at_first, at_last = lane == 0, lane == cells - 1
    left = halo[0] * jnp.where(me > 0, 1.0, 0.0)
    right = halo[1] * jnp.where(me < devices - 1, 1.0, 0.0)

    def wet_of(slot):
        return jnp.where(slot < length, wet[slot], 0).astype(jnp.float32)

    def block_of(slot, mask):
        return received[rows[lax.rem(slot, devices)] + lax.div(slot, devices)] * mask

    ahead = jnp.maximum(base - 1, 0)
    before = jnp.where(base == 0, left, block_of(ahead, wet_of(ahead)))
    mask = wet_of(base)
    here = block_of(base, mask)

    def one(offset, carry):
        before, here, mask = carry
        slot = base + offset
        later = jnp.minimum(slot + 1, capacity - 1)
        later_mask = wet_of(later)
        after = jnp.where(slot + 1 == length, right, block_of(later, later_mask))
        low = pltpu.roll(jnp.where(at_last, before, here), 1, 1)
        high = pltpu.roll(jnp.where(at_first, after, here), cells - 1, 1)
        out[offset] = (low + high + 2.0 * here) * (scale * mask)
        return here, after, later_mask

    lax.fori_loop(0, chunk, one, (before, here, mask), unroll=8)


def choose_kernel(sizes, rooms, spans, out):
    groups, chips, layers = sizes
    devices = groups * chips
    plane = chips // layers
    most = jnp.int32(0)
    for layer in range(layers):
        need = jnp.int32(0)
        for grp in range(groups):
            low = grp * chips + layer * plane
            part = lax.fori_loop(0, plane, lambda i, s, low=low: s + spans[low + i], jnp.int32(0))
            need = need + lax.div(part + devices - 1, devices)
        most = jnp.maximum(most, need)
    choice = jnp.int32(0)
    for room in rooms:
        choice = choice + jnp.where(most > room, 1, 0)
    out[0] = choice


def on_device(accum, step_count, stretch_slot, span_length, wet_mask):
    groups, chips = lax.axis_size("grp"), lax.axis_size("dev")
    devices = groups * chips
    blocks_dev, fields, cells = accum.shape
    capacity = wet_mask.shape[0]
    pair_most = capacity // devices
    all_blocks = stretch_slot.shape[0]
    layers = 4 if chips % 4 == 0 else 1
    smem = pl.BlockSpec(memory_space=pltpu.SMEM)
    vmem = pl.BlockSpec(memory_space=pltpu.VMEM)
    hbm = pl.BlockSpec(memory_space=pl.ANY)
    block = (fields, cells)
    f32 = jnp.float32
    sems = pltpu.SemaphoreType.DMA
    rows = pltpu.VMEM((capacity, *block), f32)
    pair = pltpu.VMEM((2, *block), f32)
    operands = (stretch_slot, span_length, wet_mask, accum)
    sizes = (groups, chips, layers, pair_most, blocks_dev, all_blocks)

    def exchange(kernel, scratch, number):
        return pl.pallas_call(
            kernel,
            out_shape=(
                jax.ShapeDtypeStruct((capacity, *block), f32),
                jax.ShapeDtypeStruct((2, *block), f32),
            ),
            in_specs=[smem, smem, smem, vmem],
            out_specs=(hbm, hbm),
            scratch_shapes=scratch,
            compiler_params=pltpu.CompilerParams(collective_id=number, has_side_effects=True),
        )

    def direct(*given):
        scratch = [pltpu.SMEM((devices,), jnp.int32), rows, rows, pair, pair]
        scratch += [sems((devices,))] * 3 + [sems((2,)), sems((2,)), sems]
        return exchange(functools.partial(exchange_kernel, sizes), scratch, 0)(*given)

    def relay(number, room):
        def run(*given):
            one = pltpu.VMEM((room, *block), f32)
            rests = devices // layers
            scratch = [pltpu.SMEM((devices + 1,), jnp.int32), pltpu.VMEM((3, room, *block), f32)]
            scratch += [one, one, one, pltpu.VMEM((4 * rests * pair_most, *block), f32), rows, pair, pair]
            scratch += [sems((3,)), sems((3,)), sems((4 * rests,)), sems((devices,)), sems((devices,))]
            scratch += [sems((2,)), sems((2,)), sems]
            return exchange(functools.partial(relay_kernel, sizes, room), scratch, number)(*given)

        return run

    if layers == 4 and groups == 2 and pair_most >= 8:
        most = (devices // layers) * pair_most
        rooms = [most * part // 64 for part in ROOMS]
        choice = pl.pallas_call(
            functools.partial(choose_kernel, (groups, chips, layers), rooms),
            out_shape=jax.ShapeDtypeStruct((1,), jnp.int32),
            in_specs=[smem],
            out_specs=smem,
        )(span_length)[0]
        branches = [relay(number + 1, room) for number, room in enumerate(rooms)] + [direct]
        received, halo = lax.switch(choice, branches, *operands)
    else:
        received, halo = direct(*operands)
    chunk = 32 if capacity % 32 == 0 else capacity
    return pl.pallas_call(
        functools.partial(
            filter_kernel, (groups, chips, pair_most, blocks_dev, all_blocks), chunk
        ),
        grid=(capacity // chunk,),
        out_shape=jax.ShapeDtypeStruct((capacity, *block), f32),
        in_specs=[smem, smem, smem, smem, vmem, vmem],
        out_specs=pl.BlockSpec((chunk, *block), lambda step: (step, 0, 0)),
        scratch_shapes=[pltpu.SMEM((devices,), jnp.int32), pltpu.VMEM(block, f32)],
    )(stretch_slot, span_length, wet_mask, step_count, received, halo)


def solution(mesh):
    return jax.shard_map(
        on_device,
        mesh=mesh,
        in_specs=(P(("grp", "dev"), None, None), P(), P(), P(), P(("grp", "dev"))),
        out_specs=P(("grp", "dev"), None, None),
        check_vma=False,
    )
```

```python
import functools
import jax
import jax.numpy as jnp
from jax import lax
from jax.experimental import pallas as pl
from jax.experimental.pallas import tpu as pltpu
from jax.sharding import PartitionSpec as P

MESH = pl.DeviceIdType.MESH
ROOMS = (36, 38, 40, 42, 44, 48)


def exchange_kernel(
    sizes, stretch, spans, wet, accum, received, halo,
    starts, packed, landed, edge_out, edge_in, send_sem, recv_sem, out_sem, edge_send, edge_recv, edge_copy,
):
    groups, chips, layers, pair_most, blocks_dev, all_blocks = sizes
    devices = groups * chips
    plane = chips // layers
    grp = lax.axis_index("grp")
    dev = lax.axis_index("dev")
    me = grp * chips + dev
    layer, place = dev // plane, dev % plane

    def at(index):
        return (index // chips, index % chips)

    barrier = pltpu.get_barrier_semaphore()

    @pl.loop(1, devices)
    def _(step):
        pl.semaphore_signal(barrier, inc=1, device_id=at((me + step) % devices), device_id_type=MESH)

    def prefix(owner, total):
        starts[owner] = total
        return total + spans[owner]

    lax.fori_loop(0, devices, prefix, jnp.int32(0))

    def find(block, found):
        return jnp.where(stretch[block] // blocks_dev == me, block, found)

    phase = lax.fori_loop(0, devices, find, jnp.int32(0), unroll=8)

    def partner(turn, rest):
        there = ((layer + turn) % layers) * plane + (place + rest % plane) % plane
        return ((grp + rest // plane) % groups) * chips + there

    def pack(owner, target, base):
        start = starts[owner]
        first = start + lax.rem(phase - start + all_blocks * devices, devices)
        for rank in range(pair_most):
            block = jnp.minimum(first + rank * devices, all_blocks - 1)
            slot = lax.rem(stretch[block], blocks_dev)
            target[base + rank] = accum[slot]

    def send_copy(other):
        return pltpu.make_async_remote_copy(
            src_ref=packed.at[pl.ds(other * pair_most, pair_most)],
            dst_ref=landed.at[pl.ds(me * pair_most, pair_most)],
            send_sem=send_sem.at[other],
            recv_sem=recv_sem.at[me],
            device_id=at(other),
            device_id_type=MESH,
        )

    def out_copy(other):
        return pltpu.make_async_copy(
            landed.at[pl.ds(other * pair_most, pair_most)],
            received.at[pl.ds(other * pair_most, pair_most)],
            out_sem.at[other],
        )

    turns = [layers // 2] + [t for t in range(1, layers) if t != layers // 2]
    if layers > 1:
        turns = turns + [0]
    else:
        turns = [0]
    rests = groups * plane
    for number, turn in enumerate(turns):
        low = 1 if turn == 0 else 0

        @pl.loop(low, rests)
        def _(rest):
            other = partner(turn, rest)
            pack(other, packed, other * pair_most)

        if number == 0:
            pl.semaphore_wait(barrier, devices - 1)

        @pl.loop(low, rests)
        def _(rest):
            send_copy(partner(turn, rest)).start()

    pack(me, landed, me * pair_most)

    for turn in reversed(turns):
        low = 1 if turn == 0 else 0

        @pl.loop(low, rests)
        def _(rest):
            other = partner(turn, rest)
            pltpu.make_async_remote_copy(
                src_ref=packed.at[pl.ds(other * pair_most, pair_most)],
                dst_ref=landed.at[pl.ds(other * pair_most, pair_most)],
                send_sem=send_sem.at[other],
                recv_sem=recv_sem.at[other],
                device_id=at(other),
                device_id_type=MESH,
            ).wait_recv()
            out_copy(other).start()

    out_copy(me).start()

    start = starts[me]
    length = spans[me]
    first_from = stretch[start] // blocks_dev
    last = jnp.maximum(length - 1, 0)
    last_from = stretch[start + last] // blocks_dev
    edge_out[0] = landed[last_from * pair_most + last // devices] * (
        wet[last] == 1
    ).astype(jnp.float32)
    edge_out[1] = landed[first_from * pair_most] * (wet[0] == 1).astype(jnp.float32)
    copies = []
    for side, shift in ((0, 1), (1, devices - 1)):
        copies.append(
            pltpu.make_async_remote_copy(
                src_ref=edge_out.at[side],
                dst_ref=edge_in.at[side],
                send_sem=edge_send.at[side],
                recv_sem=edge_recv.at[side],
                device_id=at((me + shift) % devices),
                device_id_type=MESH,
            )
        )
    for copy in copies:
        copy.start()

    @pl.loop(1, devices)
    def _(step):
        send_copy((me + step) % devices).wait_send()

    @pl.loop(0, devices)
    def _(other):
        out_copy(other).wait()

    for copy in copies:
        copy.wait()
    final = pltpu.make_async_copy(edge_in, halo, edge_copy)
    final.start()
    final.wait()


def relay_kernel(
    sizes, room, stretch, spans, wet, accum, received, halo,
    starts, packed, relay_one, relay_two, relay_three, forward, landed, edge_out, edge_in,
    far_send, far_recv, send_sem, recv_sem, out_sem, edge_send, edge_recv, edge_copy,
):
    groups, chips, layers, pair_most, blocks_dev, all_blocks = sizes
    devices = groups * chips
    plane = chips // layers
    rests = groups * plane
    relayed = (None, relay_one, relay_two, relay_three)
    grp = lax.axis_index("grp")
    dev = lax.axis_index("dev")
    me = grp * chips + dev
    layer, place = dev // plane, dev % plane
    across = (layer, layer + 1 - 2 * (layer % 2), (layer + 2) % 4, 3 - layer)

    def at(index):
        return (index // chips, index % chips)

    barrier = pltpu.get_barrier_semaphore()

    @pl.loop(1, devices)
    def _(step):
        pl.semaphore_signal(barrier, inc=1, device_id=at((me + step) % devices), device_id_type=MESH)

    def prefix(owner, total):
        starts[owner] = total
        return total + spans[owner]

    starts[devices] = lax.fori_loop(0, devices, prefix, jnp.int32(0))

    def find(block, found):
        holder = stretch[block] // blocks_dev
        base = grp * chips + place
        return tuple(
            jnp.where(holder == base + across[turn] * plane, block, found[turn]) for turn in range(4)
        )

    phases = lax.fori_loop(0, devices, find, (jnp.int32(0),) * 4, unroll=8)

    def first_of(phase, start):
        return start + lax.rem(phase - start + all_blocks * devices, devices)

    def ranges(phase, target):
        firsts, amount = [], None
        for part in range(2):
            low = part * chips + target * plane
            first = first_of(phase, starts[low])
            firsts.append(first)
            if part == 0:
                amount = (starts[low + plane] - first + devices - 1) // devices
        return firsts, amount

    def slot_of(block):
        return lax.rem(stretch[jnp.minimum(block, all_blocks - 1)], blocks_dev)

    def far_copy(turn):
        return pltpu.make_async_remote_copy(
            src_ref=packed.at[turn - 1],
            dst_ref=relayed[turn],
            send_sem=far_send.at[turn - 1],
            recv_sem=far_recv.at[turn - 1],
            device_id=at(grp * chips + across[turn] * plane + place),
            device_id_type=MESH,
        )

    for turn in (1, 2, 3):
        (first_low, first_high), amount = ranges(phases[0], across[turn])

        def fill(spot, carry, turn=turn, first_low=first_low, first_high=first_high, amount=amount):
            block = jnp.where(
                spot < amount, first_low + devices * spot, first_high + devices * (spot - amount)
            )
            packed[turn - 1, spot] = accum[slot_of(block)]
            return carry

        lax.fori_loop(0, room, fill, jnp.int32(0), unroll=2)
        if turn == 1:
            pl.semaphore_wait(barrier, devices - 1)
        far_copy(turn).start()

    def mate(rest):
        return ((grp + rest // plane) % groups) * chips + layer * plane + (place + rest % plane) % plane

    def shifted(index, turn):
        return index + (across[turn] - layer) * plane

    def near_copy(turn, rest, sender):
        return pltpu.make_async_remote_copy(
            src_ref=forward.at[pl.ds((turn * rests + rest) * pair_most, pair_most)],
            dst_ref=landed.at[pl.ds(sender * pair_most, pair_most)],
            send_sem=send_sem.at[turn * rests + rest],
            recv_sem=recv_sem.at[sender],
            device_id=at(mate(rest)),
            device_id_type=MESH,
        )

    def out_copy(other):
        return pltpu.make_async_copy(
            landed.at[pl.ds(other * pair_most, pair_most)],
            received.at[pl.ds(other * pair_most, pair_most)],
            out_sem.at[other],
        )

    def hand_on(turn):
        phase = phases[turn]
        sender = shifted(me, turn)
        if turn > 0:
            (first_low, first_high), amount = ranges(phase, layer)

        def put(owner, target, base):
            first = first_of(phase, starts[owner])
            if turn == 0:
                for rank in range(pair_most):
                    target[base + rank] = accum[slot_of(first + rank * devices)]
            else:
                in_low = owner < chips
                spot = jnp.where(in_low, first - first_low, first - first_high) // devices
                spot = spot + jnp.where(in_low, 0, amount)
                for rank in range(pair_most):
                    target[base + rank] = relayed[turn][jnp.clip(spot + rank, 0, room - 1)]

        put(mate(1), forward, (turn * rests + 1) * pair_most)

        @pl.loop(2, rests)
        def _(rest):
            put(mate(rest), forward, (turn * rests + rest) * pair_most)
            near_copy(turn, rest - 1, sender).start()

        put(me, landed, sender * pair_most)
        near_copy(turn, rests - 1, sender).start()

    def take(turn):
        out_copy(shifted(me, turn)).start()

        @pl.loop(1, rests)
        def _(rest):
            sender = shifted(mate(rest), turn)
            near_copy(turn, rest, sender).wait_recv()
            out_copy(sender).start()

    hand_on(0)
    for turn in (1, 2, 3):
        far_copy(turn).wait_recv()
        hand_on(turn)
        take(turn - 1)
    take(3)

    start = starts[me]
    length = spans[me]
    first_from = stretch[start] // blocks_dev
    last = jnp.maximum(length - 1, 0)
    last_from = stretch[start + last] // blocks_dev
    edge_out[0] = landed[last_from * pair_most + last // devices] * (
        wet[last] == 1
    ).astype(jnp.float32)
    edge_out[1] = landed[first_from * pair_most] * (wet[0] == 1).astype(jnp.float32)
    copies = []
    for side, shift in ((0, 1), (1, devices - 1)):
        copies.append(
            pltpu.make_async_remote_copy(
                src_ref=edge_out.at[side],
                dst_ref=edge_in.at[side],
                send_sem=edge_send.at[side],
                recv_sem=edge_recv.at[side],
                device_id=at((me + shift) % devices),
                device_id_type=MESH,
            )
        )
    for copy in copies:
        copy.start()
    for turn in range(4):
        if turn > 0:
            far_copy(turn).wait_send()

        @pl.loop(1, rests)
        def _(rest):
            near_copy(turn, rest, me).wait_send()

    @pl.loop(0, devices)
    def _(other):
        out_copy(other).wait()

    for copy in copies:
        copy.wait()
    final = pltpu.make_async_copy(edge_in, halo, edge_copy)
    final.start()
    final.wait()


def filter_kernel(sizes, chunk, stretch, spans, wet, counts, received, halo, out, rows, recips):
    groups, chips, pair_most, blocks_dev, all_blocks = sizes
    devices = groups * chips
    me = lax.axis_index("grp") * chips + lax.axis_index("dev")
    step = pl.program_id(0)
    length = spans[me]
    capacity = wet.shape[0]
    _, fields, cells = halo.shape

    @pl.when(step == 0)
    def _():
        start = lax.fori_loop(
            0, devices, lambda o, s: s + jnp.where(o < me, spans[o], 0), jnp.int32(0), unroll=8
        )

        def fill(spot, carry):
            rows[spot] = (stretch[jnp.minimum(start + spot, all_blocks - 1)] // blocks_dev) * pair_most
            return carry

        lax.fori_loop(0, devices, fill, jnp.int32(0), unroll=8)
        field = lax.broadcasted_iota(jnp.int32, (fields, cells), 0)
        held = jnp.ones((fields, cells), jnp.int32)
        for index in range(fields):
            held = jnp.where(field == index, counts[index], held)
        recips[...] = 0.25 / held.astype(jnp.float32)

    base = step * chunk
    scale = recips[...]
    lane = lax.broadcasted_iota(jnp.int32, (fields, cells), 1)
    at_first, at_last = lane == 0, lane == cells - 1
    left = halo[0] * jnp.where(me > 0, 1.0, 0.0)
    right = halo[1] * jnp.where(me < devices - 1, 1.0, 0.0)

    def wet_of(slot):
        return jnp.where(slot < length, wet[slot], 0).astype(jnp.float32)

    def block_of(slot, mask):
        return received[rows[lax.rem(slot, devices)] + lax.div(slot, devices)] * mask

    ahead = jnp.maximum(base - 1, 0)
    before = jnp.where(base == 0, left, block_of(ahead, wet_of(ahead)))
    mask = wet_of(base)
    here = block_of(base, mask)

    def one(offset, carry):
        before, here, mask = carry
        slot = base + offset
        later = jnp.minimum(slot + 1, capacity - 1)
        later_mask = wet_of(later)
        after = jnp.where(slot + 1 == length, right, block_of(later, later_mask))
        low = pltpu.roll(jnp.where(at_last, before, here), 1, 1)
        high = pltpu.roll(jnp.where(at_first, after, here), cells - 1, 1)
        out[offset] = (low + high + 2.0 * here) * (scale * mask)
        return here, after, later_mask

    lax.fori_loop(0, chunk, one, (before, here, mask), unroll=8)


def choose_kernel(sizes, rooms, spans, out):
    groups, chips, layers = sizes
    devices = groups * chips
    plane = chips // layers
    most = jnp.int32(0)
    for layer in range(layers):
        need = jnp.int32(0)
        for grp in range(groups):
            low = grp * chips + layer * plane
            part = lax.fori_loop(0, plane, lambda i, s, low=low: s + spans[low + i], jnp.int32(0))
            need = need + lax.div(part + devices - 1, devices)
        most = jnp.maximum(most, need)
    choice = jnp.int32(0)
    for room in rooms:
        choice = choice + jnp.where(most > room, 1, 0)
    out[0] = choice


def on_device(accum, step_count, stretch_slot, span_length, wet_mask):
    groups, chips = lax.axis_size("grp"), lax.axis_size("dev")
    devices = groups * chips
    blocks_dev, fields, cells = accum.shape
    capacity = wet_mask.shape[0]
    pair_most = capacity // devices
    all_blocks = stretch_slot.shape[0]
    layers = 4 if chips % 4 == 0 else 1
    smem = pl.BlockSpec(memory_space=pltpu.SMEM)
    vmem = pl.BlockSpec(memory_space=pltpu.VMEM)
    hbm = pl.BlockSpec(memory_space=pl.ANY)
    block = (fields, cells)
    f32 = jnp.float32
    sems = pltpu.SemaphoreType.DMA
    rows = pltpu.VMEM((capacity, *block), f32)
    pair = pltpu.VMEM((2, *block), f32)
    operands = (stretch_slot, span_length, wet_mask, accum)
    sizes = (groups, chips, layers, pair_most, blocks_dev, all_blocks)

    def exchange(kernel, scratch, number):
        return pl.pallas_call(
            kernel,
            out_shape=(
                jax.ShapeDtypeStruct((capacity, *block), f32),
                jax.ShapeDtypeStruct((2, *block), f32),
            ),
            in_specs=[smem, smem, smem, vmem],
            out_specs=(hbm, hbm),
            scratch_shapes=scratch,
            compiler_params=pltpu.CompilerParams(collective_id=number, has_side_effects=True),
        )

    def direct(*given):
        scratch = [pltpu.SMEM((devices,), jnp.int32), rows, rows, pair, pair]
        scratch += [sems((devices,))] * 3 + [sems((2,)), sems((2,)), sems]
        return exchange(functools.partial(exchange_kernel, sizes), scratch, 0)(*given)

    def relay(number, room):
        def run(*given):
            one = pltpu.VMEM((room, *block), f32)
            rests = devices // layers
            scratch = [pltpu.SMEM((devices + 1,), jnp.int32), pltpu.VMEM((3, room, *block), f32)]
            scratch += [one, one, one, pltpu.VMEM((4 * rests * pair_most, *block), f32), rows, pair, pair]
            scratch += [sems((3,)), sems((3,)), sems((4 * rests,)), sems((devices,)), sems((devices,))]
            scratch += [sems((2,)), sems((2,)), sems]
            return exchange(functools.partial(relay_kernel, sizes, room), scratch, number)(*given)

        return run

    if layers == 4 and groups == 2 and pair_most >= 8:
        most = (devices // layers) * pair_most
        rooms = [most * part // 64 for part in ROOMS]
        choice = pl.pallas_call(
            functools.partial(choose_kernel, (groups, chips, layers), rooms),
            out_shape=jax.ShapeDtypeStruct((1,), jnp.int32),
            in_specs=[smem],
            out_specs=smem,
        )(span_length)[0]
        branches = [relay(number + 1, room) for number, room in enumerate(rooms)] + [direct]
        received, halo = lax.switch(choice, branches, *operands)
    else:
        received, halo = direct(*operands)
    chunk = 32 if capacity % 32 == 0 else capacity
    return pl.pallas_call(
        functools.partial(
            filter_kernel, (groups, chips, pair_most, blocks_dev, all_blocks), chunk
        ),
        grid=(capacity // chunk,),
        out_shape=jax.ShapeDtypeStruct((capacity, *block), f32),
        in_specs=[smem, smem, smem, smem, vmem, vmem],
        out_specs=pl.BlockSpec((chunk, *block), lambda step: (step, 0, 0)),
        scratch_shapes=[pltpu.SMEM((devices,), jnp.int32), pltpu.VMEM(block, f32)],
    )(stretch_slot, span_length, wet_mask, step_count, received, halo)


def solution(mesh):
    return jax.shard_map(
        on_device,
        mesh=mesh,
        in_specs=(P(("grp", "dev"), None, None), P(), P(), P(), P(("grp", "dev"))),
        out_specs=P(("grp", "dev"), None, None),
        check_vma=False,
    )
```
